32 devices in a mesh: groups: 2 (over x), seq: 16 (over z, y, core).
Axes of the slice: x: 2, y: 2, z: 4, core: 2. Of those that a mesh axis runs over, the one named last changes fastest.
Arguments:
- activations: bfloat16 [512, 14336], P(('groups', 'seq')), parts along dimension 0, may hold values from -6 to 6
- out_grads: bfloat16 [512, 2048], P(('groups', 'seq')), parts along dimension 0, may hold values from -6 to 6
- query_ids: int32 [512], P(('groups', 'seq')), parts along dimension 0, may hold values from 0 to 2, never falling along the last dimension, each value on 1 to 128 neighbouring positions
- act_basis: bfloat16 [64, 224, 224], P('seq'), may hold values from -0.375 to 0.375
- grad_basis: bfloat16 [2048, 2048], P(None, 'seq'), may hold values from -0.125 to 0.125
- eigenvalues: float32 [2048, 14336], P(None, 'seq'), may hold values from 8 to 80
Outputs:
- precond: bfloat16 [6, 2048, 14336], P('groups', None, 'seq'), parts along dimension 0
The draws below stay inside these ranges and needn't reach their ends.
There are 2 independent parts, one for each index of `groups`. The reference program is written for one: setup_inputs(seed, part) draws one part's arguments, and reference() takes and returns one part's arrays. A program takes and returns all parts, laid end to end along the dimension named above; an argument that names none is the same for every part. Nothing has to cross between parts.
Inputs may be any that keep to these rules, and one draw needn't show every extreme that they name: `query_ids`: query ids never fall along the tokens; each of the 3 queries has at least one and at most 128 tokens.
All inputs are finite; a program needn't handle non-finite values.
Results may differ from the reference program's by a relative error of at most 0.006.
Values may be sent and summed in bfloat16 or wider, within the bound.
A program may use at most 128 MiB of HBM per device.

```python
import math
import jax
import jax.numpy as jnp
import numpy as np

D = 2048
FF = 14336
FB = 224
QUERIES = 3
TOKENS = 256
BLOCKS = 64


def level_of(key, dims, shards, least, largest):
    factor_of, own = 1.0, jax.random.fold_in(key, 6)
    for position, shards_of in shards:
        steps = jnp.exp(jax.random.uniform(jax.random.fold_in(own, position), (shards_of,), jnp.float32, least / len(shards), largest / len(shards)))
        factor_of = factor_of * jnp.repeat(steps, dims[position] // shards_of).reshape([-1 if axis == position else 1 for axis in range(len(dims))])
    return factor_of


def profile(count, total, reach, slope):
    weights = [(1 << 20) // math.isqrt(standing ** slope) + 1 for standing in range(2, count + 1)]
    spare, given = total - reach - (count - 1), [1] * (count - 1)
    while spare > 0:
        free = [i for i in range(count - 1) if given[i] < reach]
        mass, remaining = sum([weights[i] for i in free]), spare
        for i in free:
            more = min(reach - given[i], max(1, remaining * weights[i] // mass), spare)
            given[i] = given[i] + more
            spare = spare - more
    return np.array([reach] + given)


def ragged(rng, amount, total, reach, skew):
    if amount == 2:
        one = jax.random.randint(rng, (), max(1, total - reach), min(reach, total - 1) + 1)
        return jnp.stack([one, total - one])
    tallies = jnp.asarray(profile(amount, total, reach, skew), jnp.int32)
    couples = (amount - 1) // 2
    donor, sink = tallies[1:1 + 2 * couples:2], tallies[2:2 + 2 * couples:2]
    room = jnp.minimum(donor - 1, reach - sink)
    passed = jax.random.randint(jax.random.fold_in(rng, 1), (couples,), 0, 1 << 20) % (room + 1)
    tallies = tallies.at[1:1 + 2 * couples:2].set(donor - passed).at[2:2 + 2 * couples:2].set(sink + passed)
    return tallies[jax.random.permutation(jax.random.fold_in(rng, 2), amount)]


def normal_values(rng, extent, spread, most, pieces=(), held_as=jnp.bfloat16):
    gain = level_of(rng, extent, pieces, -0.22, 0.18) if pieces else 1.0
    entries = jax.random.normal(rng, extent, jnp.float32) * spread * gain
    return jnp.minimum(jnp.maximum(entries, -most), most).astype(held_as)


def setup_inputs(seed: int = 0, part: int = 0) -> dict:
    seeds = jax.random.split(jax.random.key(seed), 7)
    part_splits = jax.random.split(jax.random.fold_in(seeds[6], part), 7)
    activations = normal_values(part_splits[0], (TOKENS, FF), 1.0, 6.0, ((0, 16),))
    out_grads = normal_values(part_splits[1], (TOKENS, D), 1.0, 6.0, ((0, 16),))
    query_ids = jnp.searchsorted(jnp.cumsum(ragged(part_splits[2], QUERIES, TOKENS, TOKENS // 2, 0)), jnp.arange(TOKENS), side="right").astype(jnp.int32)
    act_basis = normal_values(seeds[3], (BLOCKS, FB, FB), FB ** -0.5, 0.375, ((0, 16),))
    grad_basis = normal_values(seeds[4], (D, D), D ** -0.5, 0.125, ((1, 16),))
    eigenvalues = jnp.clip(jnp.exp(math.log(80.0) - 2.3025851 * jax.random.uniform(seeds[5], (D, FF), jnp.float32) ** level_of(seeds[5], (D, FF), ((1, 16),), -0.2, 0.2)), 8.0, 80.0)
    return dict(activations=activations, out_grads=out_grads, query_ids=query_ids, act_basis=act_basis, grad_basis=grad_basis, eigenvalues=eigenvalues)


def reference(activations, out_grads, query_ids, act_basis, grad_basis, eigenvalues):
    all_tokens = activations.shape[0]
    blocks = act_basis.shape[0]
    block_order = act_basis.shape[1]
    out_units = grad_basis.shape[0]
    basis_wide = act_basis.astype(jnp.float32)
    rotated_act = jnp.einsum("tbi,bik->tbk", activations.reshape(all_tokens, blocks, block_order).astype(jnp.float32), basis_wide)
    rotated_act = rotated_act.astype(jnp.bfloat16).reshape(all_tokens, blocks * block_order)
    rotated_grad = jnp.dot(out_grads, grad_basis, preferred_element_type=jnp.float32).astype(jnp.bfloat16)
    outputs = []
    for query_index in range(QUERIES):
        selected = jnp.where((query_ids == query_index)[:, None], rotated_act, jnp.zeros_like(rotated_act))
        moments = jnp.dot(rotated_grad.T, selected, preferred_element_type=jnp.float32)
        scaled = (moments / eigenvalues).astype(jnp.bfloat16)
        rotated_back = jnp.einsum("dbk,bik->dbi", scaled.reshape(out_units, blocks, block_order).astype(jnp.float32), basis_wide)
        rotated_back = rotated_back.astype(jnp.bfloat16).reshape(out_units, blocks * block_order)
        outputs.append(jnp.dot(grad_basis, rotated_back, preferred_element_type=jnp.float32).astype(jnp.bfloat16))
    return jnp.stack(outputs, axis=0)
```

```python
import functools

import jax
import jax.numpy as jnp
from jax import lax
from jax.experimental import pallas as pl
from jax.experimental.pallas import tpu as pltpu
from jax.sharding import PartitionSpec as P

QUERIES = 3
LANES = 128
TILE = 256


def bands(width, order):
    out = []
    for start in range(0, width, TILE):
        stop = min(start + TILE, width)
        low = start // order * order // LANES * LANES
        high = min(width, -(-(((stop - 1) // order + 1) * order) // LANES) * LANES)
        out.append((start, stop, low, high))
    return out


def back_kernel(order, basis_ref, grads_ref, act_ref, ids_ref, eig_ref, turn_ref, out_ref):
    rotated = jnp.dot(grads_ref[...], basis_ref[...], preferred_element_type=jnp.float32)
    rotated = rotated.astype(jnp.bfloat16)
    act = act_ref[...]
    ids = ids_ref[...]
    for query in range(QUERIES):
        selected = act * (ids == query).astype(jnp.bfloat16)
        moments = lax.dot_general(
            rotated, selected, (((0,), (0,)), ((), ())), preferred_element_type=jnp.float32
        )
        scaled = (moments / eig_ref[...]).astype(jnp.bfloat16)
        for start, stop, low, high in bands(act.shape[1], order):
            out_ref[query, :, start:stop] = jnp.dot(
                scaled[:, low:high], turn_ref[low:high, start:stop], preferred_element_type=jnp.float32
            ).astype(jnp.bfloat16)


def final_kernel(chunks, *refs):
    basis, back, out_ref = refs[:chunks], refs[chunks : 2 * chunks], refs[-1]
    total = None
    for g, b in zip(basis, back):
        term = jnp.dot(g[...], b[0], preferred_element_type=jnp.float32)
        total = term if total is None else total + term
    out_ref[0] = total.astype(jnp.bfloat16)


def shards(groups, n, activations, out_grads, query_ids, act_basis, grad_basis, eigenvalues):
    own_tokens = activations.shape[0]
    blocks, order = act_basis.shape[:2]
    units, cols = grad_basis.shape
    width = blocks * order
    tokens = own_tokens * n
    outer = n // 4
    me, group = lax.axis_index("seq"), lax.axis_index("groups")
    z, y, c = me // 4, me // 2 % 2, me % 2

    ring = [(i, (i + 4) % n) for i in range(n)]
    side = [(i, i ^ 2) for i in range(n)]
    core = [(i, i ^ 1) for i in range(n)]

    pieces = [grad_basis]
    for _ in range(outer - 1):
        pieces.append(lax.ppermute(pieces[-1], "seq", ring))
    chunks, eigs = [], []
    for step, piece in enumerate(pieces):
        if groups == 2 and units % 32 == 0:
            half = units // 2
            sent = lax.dynamic_slice_in_dim(piece, group * half, half, axis=0)
            mine = lax.ppermute(sent, "seq", side)
            theirs = lax.ppermute(mine, "groups", [(0, 1), (1, 0)])
            first = group == 0
            other = jnp.concatenate(
                [jnp.where(first, mine, theirs), jnp.where(first, theirs, mine)], axis=0
            )
        else:
            other = lax.ppermute(piece, "seq", side)
        pair = jnp.concatenate([piece, other], axis=1)
        chunks.append(jnp.concatenate([pair, lax.ppermute(pair, "seq", core)], axis=1))
        level = (z - step) % outer * 4
        origins = [level + yy * 2 + cc for cc in (c, 1 - c) for yy in (y, 1 - y)]
        eigs.append(
            jnp.concatenate(
                [lax.dynamic_slice_in_dim(eigenvalues, o * cols, cols, axis=0) for o in origins], axis=0
            )
        )

    ids = jnp.broadcast_to(query_ids.astype(jnp.bfloat16)[:, None, None], (own_tokens, n, LANES))
    sent = jnp.concatenate([activations.reshape(own_tokens, n, width), ids], axis=2)
    columns = lax.all_to_all(
        jnp.transpose(sent, (1, 0, 2)), "seq", split_axis=0, concat_axis=0, tiled=True
    ).reshape(tokens, width + LANES)
    token_query = columns[:, width : width + 1].astype(jnp.float32)
    grads = jnp.concatenate(
        [lax.all_gather(part, "seq", axis=0, tiled=True) for part in jnp.split(out_grads, 2, axis=1)],
        axis=1,
    )

    wide = jnp.concatenate(
        [
            jnp.pad(act_basis[b], ((0, 0), (b * order, width - (b + 1) * order)))
            for b in range(blocks)
        ],
        axis=0,
    )
    turned = wide.T
    act = jnp.dot(columns[:, :width], wide, preferred_element_type=jnp.float32).astype(jnp.bfloat16)

    chunk_cols = 4 * cols
    backs = [
        pl.pallas_call(
            functools.partial(back_kernel, order),
            out_shape=jax.ShapeDtypeStruct((QUERIES, chunk_cols, width), jnp.bfloat16),
            in_specs=[pl.BlockSpec(memory_space=pltpu.VMEM)] * 6,
            out_specs=pl.BlockSpec(memory_space=pltpu.VMEM),
            compiler_params=pltpu.CompilerParams(vmem_limit_bytes=40 * 2**20),
            cost_estimate=pl.CostEstimate(
                flops=2 * chunk_cols * (tokens * units + QUERIES * width * (tokens + width // 2)),
                bytes_accessed=2 * units * (chunk_cols + tokens) + 10 * chunk_cols * width,
                transcendentals=0,
            ),
            name="back",
        )(chunk, grads, act, token_query, eig, turned)
        for chunk, eig in zip(chunks, eigs)
    ]

    rows = min(units, 512)
    return pl.pallas_call(
        functools.partial(final_kernel, outer),
        grid=(QUERIES, units // rows),
        out_shape=jax.ShapeDtypeStruct((QUERIES, units, width), jnp.bfloat16),
        in_specs=[pl.BlockSpec((rows, chunk_cols), lambda q, r: (r, 0))] * outer
        + [pl.BlockSpec((1, chunk_cols, width), lambda q, r: (q, 0, 0))] * outer,
        out_specs=pl.BlockSpec((1, rows, width), lambda q, r: (q, r, 0)),
        compiler_params=pltpu.CompilerParams(vmem_limit_bytes=40 * 2**20),
        cost_estimate=pl.CostEstimate(
            flops=2 * QUERIES * units * units * width,
            bytes_accessed=2 * units * units + 4 * QUERIES * units * width,
            transcendentals=0,
        ),
        name="final",
    )(*chunks, *backs)


def solution(mesh):
    return jax.shard_map(
        functools.partial(shards, mesh.shape["groups"], mesh.shape["seq"]),
        mesh=mesh,
        in_specs=(
            P(("groups", "seq"), None),
            P(("groups", "seq"), None),
            P(("groups", "seq")),
            P("seq", None, None),
            P(None, "seq"),
            P(None, "seq"),
        ),
        out_specs=P("groups", None, "seq"),
        check_vma=False,
    )
```

```python
import functools

import jax
import jax.numpy as jnp
from jax import lax
from jax.experimental import pallas as pl
from jax.experimental.pallas import tpu as pltpu
from jax.sharding import PartitionSpec as P

QUERIES = 3
LANES = 128
TILE = 256


def bands(width, order):
    out = []
    for start in range(0, width, TILE):
        stop = min(start + TILE, width)
        low = start // order * order // LANES * LANES
        high = min(width, -(-(((stop - 1) // order + 1) * order) // LANES) * LANES)
        out.append((start, stop, low, high))
    return out


def back_kernel(order, basis_ref, grads_ref, act_ref, ids_ref, eig_ref, turn_ref, out_ref):
    rotated = jnp.dot(grads_ref[...], basis_ref[...], preferred_element_type=jnp.float32)
    rotated = rotated.astype(jnp.bfloat16)
    act = act_ref[...]
    ids = ids_ref[...]
    for query in range(QUERIES):
        selected = act * (ids == query).astype(jnp.bfloat16)
        moments = lax.dot_general(
            rotated, selected, (((0,), (0,)), ((), ())), preferred_element_type=jnp.float32
        )
        scaled = (moments / eig_ref[...]).astype(jnp.bfloat16)
        for start, stop, low, high in bands(act.shape[1], order):
            out_ref[query, :, start:stop] = jnp.dot(
                scaled[:, low:high], turn_ref[low:high, start:stop], preferred_element_type=jnp.float32
            ).astype(jnp.bfloat16)


def final_kernel(chunks, *refs):
    basis, back, out_ref = refs[:chunks], refs[chunks : 2 * chunks], refs[-1]
    total = None
    for g, b in zip(basis, back):
        term = jnp.dot(g[...], b[0], preferred_element_type=jnp.float32)
        total = term if total is None else total + term
    out_ref[0] = total.astype(jnp.bfloat16)


def shards(groups, n, activations, out_grads, query_ids, act_basis, grad_basis, eigenvalues):
    own_tokens = activations.shape[0]
    blocks, order = act_basis.shape[:2]
    units, cols = grad_basis.shape
    width = blocks * order
    tokens = own_tokens * n
    outer = n // 4
    me, group = lax.axis_index("seq"), lax.axis_index("groups")
    z, y, c = me // 4, me // 2 % 2, me % 2

    ring = [(i, (i + 4) % n) for i in range(n)]
    side = [(i, i ^ 2) for i in range(n)]
    core = [(i, i ^ 1) for i in range(n)]

    pieces = [grad_basis]
    for _ in range(outer - 1):
        pieces.append(lax.ppermute(pieces[-1], "seq", ring))
    chunks, eigs = [], []
    for step, piece in enumerate(pieces):
        if groups == 2 and units % 32 == 0:
            half = units // 2
            sent = lax.dynamic_slice_in_dim(piece, group * half, half, axis=0)
            mine = lax.ppermute(sent, "seq", side)
            theirs = lax.ppermute(mine, "groups", [(0, 1), (1, 0)])
            first = group == 0
            other = jnp.concatenate(
                [jnp.where(first, mine, theirs), jnp.where(first, theirs, mine)], axis=0
            )
        else:
            other = lax.ppermute(piece, "seq", side)
        pair = jnp.concatenate([piece, other], axis=1)
        chunks.append(jnp.concatenate([pair, lax.ppermute(pair, "seq", core)], axis=1))
        level = (z - step) % outer * 4
        origins = [level + yy * 2 + cc for cc in (c, 1 - c) for yy in (y, 1 - y)]
        eigs.append(
            jnp.concatenate(
                [lax.dynamic_slice_in_dim(eigenvalues, o * cols, cols, axis=0) for o in origins], axis=0
            )
        )

    ids = jnp.broadcast_to(query_ids.astype(jnp.bfloat16)[:, None, None], (own_tokens, n, LANES))
    every = jnp.broadcast_to(out_grads[:, None, :], (own_tokens, n, units))
    sent = jnp.concatenate([activations.reshape(own_tokens, n, width), ids, every], axis=2)
    columns = lax.all_to_all(
        jnp.transpose(sent, (1, 0, 2)), "seq", split_axis=0, concat_axis=0, tiled=True
    ).reshape(tokens, width + LANES + units)
    token_query = columns[:, width : width + 1].astype(jnp.float32)
    grads = columns[:, width + LANES :]

    wide = jnp.concatenate(
        [
            jnp.pad(act_basis[b], ((0, 0), (b * order, width - (b + 1) * order)))
            for b in range(blocks)
        ],
        axis=0,
    )
    turned = wide.T
    act = jnp.dot(columns[:, :width], wide, preferred_element_type=jnp.float32).astype(jnp.bfloat16)

    chunk_cols = 4 * cols
    backs = [
        pl.pallas_call(
            functools.partial(back_kernel, order),
            out_shape=jax.ShapeDtypeStruct((QUERIES, chunk_cols, width), jnp.bfloat16),
            in_specs=[pl.BlockSpec(memory_space=pltpu.VMEM)] * 6,
            out_specs=pl.BlockSpec(memory_space=pltpu.VMEM),
            compiler_params=pltpu.CompilerParams(vmem_limit_bytes=40 * 2**20),
            cost_estimate=pl.CostEstimate(
                flops=2 * chunk_cols * (tokens * units + QUERIES * width * (tokens + width // 2)),
                bytes_accessed=2 * units * (chunk_cols + tokens) + 10 * chunk_cols * width,
                transcendentals=0,
            ),
            name="back",
        )(chunk, grads, act, token_query, eig, turned)
        for chunk, eig in zip(chunks, eigs)
    ]

    rows = min(units, 512)
    return pl.pallas_call(
        functools.partial(final_kernel, outer),
        grid=(QUERIES, units // rows),
        out_shape=jax.ShapeDtypeStruct((QUERIES, units, width), jnp.bfloat16),
        in_specs=[pl.BlockSpec((rows, chunk_cols), lambda q, r: (r, 0))] * outer
        + [pl.BlockSpec((1, chunk_cols, width), lambda q, r: (q, 0, 0))] * outer,
        out_specs=pl.BlockSpec((1, rows, width), lambda q, r: (q, r, 0)),
        compiler_params=pltpu.CompilerParams(vmem_limit_bytes=40 * 2**20),
        cost_estimate=pl.CostEstimate(
            flops=2 * QUERIES * units * units * width,
            bytes_accessed=2 * units * units + 4 * QUERIES * units * width,
            transcendentals=0,
        ),
        name="final",
    )(*chunks, *backs)


def solution(mesh):
    return jax.shard_map(
        functools.partial(shards, mesh.shape["groups"], mesh.shape["seq"]),
        mesh=mesh,
        in_specs=(
            P(("groups", "seq"), None),
            P(("groups", "seq"), None),
            P(("groups", "seq")),
            P("seq", None, None),
            P(None, "seq"),
            P(None, "seq"),
        ),
        out_specs=P("groups", None, "seq"),
        check_vma=False,
    )
```
